32 devices in a mesh: dp: 8 (over z, y), tensor: 4 (over x, core).
Axes of the slice: x: 2, y: 2, z: 4, core: 2. Of those that a mesh axis runs over, the one named last changes fastest.
Arguments:
- attention_output: bfloat16 [4096, 8192], P('dp', 'tensor'), may hold values from -6 to 6
- frozen_weight: bfloat16 [8192, 8192], P('tensor'), may hold values from -0.0625 to 0.0625
- output_gradient: bfloat16 [4096, 8192], P('dp', 'tensor'), may hold values from -6 to 6
- tenant_token_count: int32 [8, 32], P('dp'), may hold values from 1 to 256, 512 in all within a row
- tenant_storage_slot: int32 [32], replicated, may hold values from 0 to 31, each once
- adapter_down_weight: float32 [32, 8192, 16], P('dp', 'tensor'), may hold values from -0.0625 to 0.0625
- adapter_up_weight: float32 [32, 16, 8192], P('dp', None, 'tensor'), may hold values from -1.5 to 1.5
- down_first_moment: float32 [32, 8192, 16], P('dp', 'tensor'), may hold values from -60 to 60
- down_second_moment: float32 [32, 8192, 16], P('dp', 'tensor'), may hold values from 1 to 10000
- up_first_moment: float32 [32, 16, 8192], P('dp', None, 'tensor'), may hold values from -60 to 60
- up_second_moment: float32 [32, 16, 8192], P('dp', None, 'tensor'), may hold values from 1 to 10000
Outputs:
- proj_out: bfloat16 [4096, 8192], P('dp', 'tensor')
- input_grad: bfloat16 [4096, 8192], P('dp', 'tensor')
- updated_down_weight: float32 [32, 8192, 16], P('dp', 'tensor')
- updated_up_weight: float32 [32, 16, 8192], P('dp', None, 'tensor')
- updated_down_first_moment: float32 [32, 8192, 16], P('dp', 'tensor')
- updated_down_second_moment: float32 [32, 8192, 16], P('dp', 'tensor')
- updated_up_first_moment: float32 [32, 16, 8192], P('dp', None, 'tensor')
- updated_up_second_moment: float32 [32, 16, 8192], P('dp', None, 'tensor')
The draws below stay inside these ranges and needn't reach their ends.
Inputs may be any that keep to these rules, and one draw needn't show every extreme that they name: `tenant_token_count`: each row sums to 512; every tenant has at least one token in every row; tokens of one dp index are sorted by tenant. `tenant_storage_slot`: a permutation of the slots.
All inputs are finite; a program needn't handle non-finite values.
Results may differ from the reference program's by a relative error of at most 0.02.
Values may be sent and summed in bfloat16 or wider, within the bound.
A program may use at most 128 MiB of HBM per device.

```python
import math
import jax
import jax.numpy as jnp
import numpy as np
from jax import lax

MODEL_WIDTH = 8192
ADAPTER_RANK = 16
TOK_DEV = 512
TENANT_TOTAL = 32
TOKENS = 4096
N_DP = 8
N_TENSOR = 4


def block_scale(stream_key, dims, cuts, low, top_value):
    factor_of, own = 1.0, jax.random.fold_in(stream_key, 6)
    for position, parts in cuts:
        steps = jnp.exp(jax.random.uniform(jax.random.fold_in(own, position), (parts,), jnp.float32, low / len(cuts), top_value / len(cuts)))
        factor_of = factor_of * jnp.repeat(steps, dims[position] // parts).reshape([-1 if axis == position else 1 for axis in range(len(dims))])
    return factor_of


def length_profile(number_of, total, limit, slope):
    loads = [(1 << 20) // math.isqrt(standing ** slope) + 1 for standing in range(2, number_of + 1)]
    rest, counts = total - limit - (number_of - 1), [1] * (number_of - 1)
    while rest > 0:
        candidates = [i for i in range(number_of - 1) if counts[i] < limit]
        mass, budget = sum([loads[i] for i in candidates]), rest
        for i in candidates:
            more = min(limit - counts[i], max(1, budget * loads[i] // mass), rest)
            counts[i] = counts[i] + more
            rest = rest - more
    return np.array([limit] + counts)


def ragged(rng, number_of, total, bound, lean):
    if number_of == 2:
        one = jax.random.randint(rng, (), max(1, total - bound), min(bound, total - 1) + 1)
        return jnp.stack([one, total - one])
    tallies = jnp.asarray(length_profile(number_of, total, bound, lean), jnp.int32)
    pairs = (number_of - 1) // 2
    giver, taker = tallies[1:1 + 2 * pairs:2], tallies[2:2 + 2 * pairs:2]
    slack = jnp.minimum(giver - 1, bound - taker)
    passed = jax.random.randint(jax.random.fold_in(rng, 1), (pairs,), 0, 1 << 20) % (slack + 1)
    tallies = tallies.at[1:1 + 2 * pairs:2].set(giver - passed).at[2:2 + 2 * pairs:2].set(taker + passed)
    return tallies[jax.random.permutation(jax.random.fold_in(rng, 2), number_of)]


def bell_draw(own_key, shape, scale, most, split=(), kind=jnp.bfloat16):
    gain = block_scale(own_key, shape, split, -0.22, 0.18) if split else 1.0
    array = jax.random.normal(own_key, shape, jnp.float32) * scale * gain
    return jnp.minimum(jnp.maximum(array, -most), most).astype(kind)


def setup_inputs(seed: int = 0) -> dict:
    keys = jax.random.split(jax.random.key(seed), 12)
    attention_output = bell_draw(keys[0], (TOKENS, MODEL_WIDTH), 1.0, 6.0, ((0, 8), (1, 4)))
    frozen_weight = bell_draw(keys[1], (MODEL_WIDTH, MODEL_WIDTH), MODEL_WIDTH ** -0.5, 0.0625, ((0, 4),))
    output_gradient = bell_draw(keys[2], (TOKENS, MODEL_WIDTH), 1.0, 6.0, ((0, 8), (1, 4)))
    tenant_token_count = jax.vmap(lambda own: ragged(own, TENANT_TOTAL, TOK_DEV, TOK_DEV // 2, 2))(jax.random.split(keys[3], N_DP)).reshape((N_DP, TENANT_TOTAL)).astype(jnp.int32)
    tenant_storage_slot = jax.random.permutation(keys[4], TENANT_TOTAL).astype(jnp.int32)
    adapter_down_weight = bell_draw(keys[5], (TENANT_TOTAL, MODEL_WIDTH, ADAPTER_RANK), MODEL_WIDTH ** -0.5, 0.0625, ((0, 8), (1, 4)), jnp.float32)
    adapter_up_weight = bell_draw(keys[6], (TENANT_TOTAL, ADAPTER_RANK, MODEL_WIDTH), ADAPTER_RANK ** -0.5, 1.5, ((0, 8), (2, 4)), jnp.float32)
    down_first_moment = bell_draw(keys[7], (TENANT_TOTAL, MODEL_WIDTH, ADAPTER_RANK), 10.0, 60.0, ((0, 8), (1, 4)), jnp.float32)
    down_second_moment = jnp.clip(jnp.exp(math.log(10000.0) - 9.2103404 * jax.random.uniform(keys[8], (TENANT_TOTAL, MODEL_WIDTH, ADAPTER_RANK), jnp.float32) ** block_scale(keys[8], (TENANT_TOTAL, MODEL_WIDTH, ADAPTER_RANK), ((0, 8), (1, 4)), -0.2, 0.2)), 1.0, 10000.0)
    up_first_moment = bell_draw(keys[9], (TENANT_TOTAL, ADAPTER_RANK, MODEL_WIDTH), 10.0, 60.0, ((0, 8), (2, 4)), jnp.float32)
    up_second_moment = jnp.clip(jnp.exp(math.log(10000.0) - 9.2103404 * jax.random.uniform(keys[10], (TENANT_TOTAL, ADAPTER_RANK, MODEL_WIDTH), jnp.float32) ** block_scale(keys[10], (TENANT_TOTAL, ADAPTER_RANK, MODEL_WIDTH), ((0, 8), (2, 4)), -0.2, 0.2)), 1.0, 10000.0)
    return {"attention_output": attention_output, "frozen_weight": frozen_weight, "output_gradient": output_gradient, "tenant_token_count": tenant_token_count, "tenant_storage_slot": tenant_storage_slot, "adapter_down_weight": adapter_down_weight, "adapter_up_weight": adapter_up_weight, "down_first_moment": down_first_moment, "down_second_moment": down_second_moment, "up_first_moment": up_first_moment, "up_second_moment": up_second_moment}


def adam_update(param, first, second, grad):
    first = 0.9 * first + 0.1 * grad
    second = 0.999 * second + 0.001 * grad * grad
    corr_one = 1.0 - 0.9 ** 10
    corr_two = 1.0 - 0.999 ** 10
    step_size = first / corr_one / (jnp.sqrt(second / corr_two) + 1e-08)
    return (param - 0.01 * (step_size + 0.1 * param), first, second)

def reference(attention_output, frozen_weight, output_gradient, tenant_token_count, tenant_storage_slot, adapter_down_weight, adapter_up_weight, down_first_moment, down_second_moment, up_first_moment, up_second_moment):
    positions = jnp.arange(TOK_DEV, dtype=jnp.int32)
    ends = jnp.cumsum(tenant_token_count, axis=1)
    tenant = lax.optimization_barrier(jnp.sum((ends[:, None, :] <= positions[None, :, None]).astype(jnp.int32), axis=-1)).reshape(-1)
    slot = tenant_storage_slot[tenant]
    onehot = (slot[:, None] == jnp.arange(TENANT_TOTAL, dtype=jnp.int32)[None, :]).astype(jnp.float32)
    down_half_precision = adapter_down_weight.astype(jnp.bfloat16)
    up_half_precision = adapter_up_weight.astype(jnp.bfloat16)
    down_flat = jnp.transpose(down_half_precision, (1, 0, 2)).reshape(MODEL_WIDTH, TENANT_TOTAL * ADAPTER_RANK)
    up_flat = up_half_precision.reshape(TENANT_TOTAL * ADAPTER_RANK, MODEL_WIDTH)
    low_all = jnp.dot(attention_output, down_flat, preferred_element_type=jnp.float32).reshape(-1, TENANT_TOTAL, ADAPTER_RANK)
    low = lax.optimization_barrier(jnp.sum(low_all * onehot[:, :, None], axis=1))
    low_wide = (onehot[:, :, None] * low[:, None, :]).reshape(-1, TENANT_TOTAL * ADAPTER_RANK).astype(jnp.bfloat16)
    width = MODEL_WIDTH // N_TENSOR

    def add_block(total, index):
        cols = lax.dynamic_slice_in_dim(attention_output, index * width, width, 1)
        rows = lax.dynamic_slice_in_dim(frozen_weight, index * width, width, 0)
        part = lax.optimization_barrier(jnp.dot(cols, rows, preferred_element_type=jnp.float32).astype(jnp.bfloat16))
        return (total + part.astype(jnp.float32), None)
    base, _ = lax.scan(add_block, jnp.zeros((TOKENS, MODEL_WIDTH), jnp.float32), jnp.arange(N_TENSOR, dtype=jnp.int32))
    proj_out = (base + 2.0 * jnp.dot(low_wide, up_flat, preferred_element_type=jnp.float32)).astype(jnp.bfloat16)
    back_all = lax.dot_general(output_gradient, up_flat, (((1,), (1,)), ((), ())), preferred_element_type=jnp.float32).reshape(-1, TENANT_TOTAL, ADAPTER_RANK)
    back = lax.optimization_barrier(jnp.sum(back_all * onehot[:, :, None], axis=1))
    back_wide = (onehot[:, :, None] * back[:, None, :]).reshape(-1, TENANT_TOTAL * ADAPTER_RANK).astype(jnp.bfloat16)
    grad_base = lax.dot_general(output_gradient, frozen_weight, (((1,), (1,)), ((), ())), preferred_element_type=jnp.float32)
    grad_low = lax.dot_general(back_wide, down_flat, (((1,), (1,)), ((), ())), preferred_element_type=jnp.float32)
    input_grad = (grad_base + 2.0 * grad_low).astype(jnp.bfloat16)
    down_gradient = 2.0 * lax.dot_general(attention_output, back_wide, (((0,), (0,)), ((), ())), preferred_element_type=jnp.float32)
    down_gradient = jnp.transpose(down_gradient.reshape(MODEL_WIDTH, TENANT_TOTAL, ADAPTER_RANK), (1, 0, 2))
    up_gradient = 2.0 * lax.dot_general(low_wide, output_gradient, (((0,), (0,)), ((), ())), preferred_element_type=jnp.float32)
    up_gradient = up_gradient.reshape(TENANT_TOTAL, ADAPTER_RANK, MODEL_WIDTH)
    updated_down_weight, updated_down_first_moment, updated_down_second_moment = adam_update(adapter_down_weight, down_first_moment, down_second_moment, down_gradient)
    updated_up_weight, updated_up_first_moment, updated_up_second_moment = adam_update(adapter_up_weight, up_first_moment, up_second_moment, up_gradient)
    return (proj_out, input_grad, updated_down_weight, updated_up_weight, updated_down_first_moment, updated_down_second_moment, updated_up_first_moment, updated_up_second_moment)
```

```python
import functools

import jax
import jax.numpy as jnp
from jax import lax
from jax.experimental import pallas as pl
from jax.experimental.pallas import tpu as pltpu
from jax.sharding import PartitionSpec as P

MESH = pl.DeviceIdType.MESH
NT = (((1,), (1,)), ((), ()))
TN = (((0,), (0,)), ((), ()))


def adam_update(param, first, second, grad):
    first = 0.9 * first + 0.1 * grad
    second = 0.999 * second + 0.001 * grad * grad
    corr_one = 1.0 - 0.9**10
    corr_two = 1.0 - 0.999**10
    step_size = first / corr_one / (jnp.sqrt(second / corr_two) + 1e-08)
    return (param - 0.01 * (step_size + 0.1 * param), first, second)


def dot(a, b, dims=(((1,), (0,)), ((), ()))):
    return lax.dot_general(a, b, dims, preferred_element_type=jnp.float32)


def step_kernel(
    n_dp, n_tensor, rank, tile,
    x_hbm, w_hbm, g_hbm, down_hbm, up_hbm, counts_ref, storage_ref,
    proj_hbm, dx_hbm, gup_hbm, gdown_hbm,
    xv, wbuf, gbuf, pbuf, rbuf, xbuf, acc, stage, adp, wide, bounds,
    eown, epart, esum, ex, part, ybuf, zbuf, obuf,
    wsem, xsem, glsem, alsem, osem, gosem,
    gxs, gxr, gds, gdr, pds, pdr, pxs, pxr,
    azs, azr, ays, ayr, eds, edr, exs, exr, rys, ryr, rzs, rzr,
):
    f32, bf16 = jnp.float32, jnp.bfloat16
    rows, width = x_hbm.shape
    chunks = width // tile
    n_tiles = n_tensor * chunks
    big_r, big_k = n_dp // 2, n_tensor // 2
    e_all, _ = adp.shape[1:]
    e_own = stage.shape[1]
    half = big_r * e_own
    owned = e_own // rank

    d, t = lax.axis_index("dp"), lax.axis_index("tensor")
    z, yc = d // 2, d % 2
    trow, core = t // 2, t % 2
    partner = (d, t + 1 - 2 * core)
    ypeer = (d + 1 - 2 * yc, t)
    left, right = (d - 2, t), (d + 2, t)
    has_l, has_r = z > 0, z < big_r - 1

    def xpeer(k):
        return (d, ((trow + k) % big_k) * 2 + core)

    def rc(src, dst, ss, rs, dev):
        return pltpu.make_async_remote_copy(
            src_ref=src, dst_ref=dst, send_sem=ss, recv_sem=rs, device_id=dev, device_id_type=MESH
        )

    def arrived(ref, sem):
        rc(ref, ref, sem, sem, partner).wait_recv()

    def tile_of(j):
        q = (j % n_tiles) // 2
        k, c, odd = q // chunks, q % chunks, j % 2
        base_row, base_core = (trow + k + 1) % big_k, jnp.where(odd == 0, 1 - core, core)
        grad_row, grad_core = (trow - k + big_k) % big_k, jnp.where(odd == 0, core, 1 - core)
        row = jnp.where(j < n_tiles, base_row, grad_row)
        side = jnp.where(j < n_tiles, base_core, grad_core)
        return (row * 2 + side) * chunks + c

    def wcopy(j):
        col = pl.multiple_of(tile_of(j) * tile, tile)
        return pltpu.make_async_copy(w_hbm.at[:, pl.ds(col, tile)], wbuf.at[j % 3], wsem.at[j % 3])

    def xload():
        return pltpu.make_async_copy(x_hbm, xv, xsem)

    def gload(c):
        return pltpu.make_async_copy(g_hbm.at[:, pl.ds(c * tile, tile)], gbuf.at[2 * c], glsem.at[c])

    def aload(a):
        return pltpu.make_async_copy((down_hbm, up_hbm)[a], stage.at[a], alsem.at[a])

    def gx(k, c):
        return rc(g_hbm.at[:, pl.ds(c * tile, tile)], gbuf.at[(k * chunks + c) * 2],
                  gxs.at[k - 1, c], gxr.at[k - 1, c], xpeer(k))

    def gd(k, c):
        slot = (k * chunks + c) * 2
        src = g_hbm.at[:, pl.ds(c * tile, tile)] if isinstance(k, int) and k == 0 else gbuf.at[slot]
        return rc(src, gbuf.at[slot + 1], gds.at[k, c], gdr.at[k, c], partner)

    def gd_wait(i):
        q = i // 2
        arrived(gbuf.at[i], gdr.at[q // chunks, q % chunks])

    def pd(q):
        return rc(pbuf.at[2 * q], rbuf.at[q], pds.at[q], pdr.at[q], partner)

    def px(k, c):
        q = (k - 1) * chunks + c
        return rc(pbuf.at[2 * q + 1], xbuf.at[q], pxs.at[q], pxr.at[q], xpeer(k))

    def block(col, row):
        return pl.ds(pl.multiple_of((col * big_r + row) * e_own, e_own), e_own)

    def az(a, way, s):
        row = z - s if way == 0 else z + s
        ref = adp.at[a, block(yc, row)]
        return rc(ref, ref, azs.at[a, way, s], azr.at[a, way, s], right if way == 0 else left)

    def ay(a, row):
        ref = adp.at[a, block(yc, row)]
        return rc(ref, ref, ays.at[a, row], ayr.at[a, row], ypeer)

    def ed(a):
        return rc(eown.at[a], epart.at[a], eds.at[a], edr.at[a], partner)

    def exc(a, k):
        return rc(esum.at[a], ex.at[a, k - 1], exs.at[a, k - 1], exr.at[a, k - 1], xpeer(k))

    def ry(a, row):
        return rc(part.at[a, block(1 - yc, row)], ybuf.at[a, row], rys.at[a, row], ryr.at[a, row], ypeer)

    def rz(a, way, s):
        row = z + s if way == 0 else z - s
        return rc(part.at[a, block(yc, row)], zbuf.at[a, way, s - 1],
                  rzs.at[a, way, s - 1], rzr.at[a, way, s - 1], right if way == 0 else left)

    def gather(a, s):
        for way in range(2):
            from_has = z - s >= 0 if way == 0 else z + s < big_r
            to_has = has_r if way == 0 else has_l
            row = z - s if way == 0 else z + s

            @pl.when(from_has)
            def _():
                if s > 0:
                    arrived(adp.at[a, block(yc, row)], azr.at[a, way, s - 1])
                if s < big_r - 1:
                    @pl.when(to_has)
                    def _():
                        az(a, way, s).start()
                if s > 0:
                    ay(a, row).start()
        if s == 0:
            ay(a, z).start()

    def mask():
        tok = lax.broadcasted_iota(jnp.int32, (e_all, rows), 1).astype(f32)
        return (bounds[0] <= tok) & (tok < bounds[1])

    def narrow(a):
        for r in range(big_r):
            arrived(adp.at[a, block(1 - yc, r)], ayr.at[a, r])
        if a == 0:
            every = dot(adp[0], xv[...], NT)
        else:
            every = dot(adp[1, :, 0:tile], gbuf[0], NT)
            for c in range(1, chunks):
                every = every + dot(adp[1, :, c * tile:(c + 1) * tile], gbuf[2 * c], NT)
        kept = jnp.where(mask(), every, 0.0).reshape(e_all // rank, rank, rows)
        eown[a] = jnp.sum(kept, axis=0)
        ed(a).start()

    def exchange(a):
        ed(a).wait_recv()
        esum[a] = eown[a] + epart[a]
        for k in range(1, big_k):
            exc(a, k).start()

    def spread(a):
        total = esum[a]
        for k in range(1, big_k):
            exc(a, k).wait_recv()
            total = total + ex[a, k - 1]
        tiled = jnp.broadcast_to(total[None], (e_all // rank, rank, rows)).reshape(e_all, rows)
        wide[a] = jnp.where(mask(), tiled, 0.0).astype(bf16)

    def partial(a, side):
        here = pl.ds(pl.multiple_of(side * half, half), half)
        lhs = wide[a, here, :]
        for c in range(chunks):
            rhs = gbuf[2 * c] if a == 0 else xv[:, c * tile:(c + 1) * tile]
            part[a, here, c * tile:(c + 1) * tile] = (2.0 * dot(lhs, rhs)).astype(bf16)

    def reduce_start(a):
        partial(a, 1 - yc)
        for s in range(big_r - 1, -1, -1):
            @pl.when(z + s < big_r)
            def _():
                ry(a, z + s).start()
            if s > 0:
                @pl.when(z - s >= 0)
                def _():
                    ry(a, z - s).start()
        partial(a, yc)

    def reduce_step(a, s):
        for way in range(2):
            there = z + s < big_r if way == 0 else z - s >= 0
            before = has_l if way == 0 else has_r
            row = z + s if way == 0 else z - s

            @pl.when(there)
            def _():
                ry(a, row).wait_recv()
                here = block(yc, row)
                if s == big_r - 1:
                    part[a, here, :] = (part[a, here, :].astype(f32) + ybuf[a, row].astype(f32)).astype(bf16)
                else:
                    @pl.when(before)
                    def _():
                        arrived(zbuf.at[a, way, s], rzr.at[a, way, s])
                        part[a, here, :] = (part[a, here, :].astype(f32) + ybuf[a, row].astype(f32)
                                            + zbuf[a, way, s].astype(f32)).astype(bf16)

                    @pl.when(jnp.logical_not(before))
                    def _():
                        part[a, here, :] = (part[a, here, :].astype(f32) + ybuf[a, row].astype(f32)).astype(bf16)
                rz(a, way, s).start()

    def reduce_end(a):
        ry(a, z).wait_recv()
        stage[a] = part[a, block(yc, z), :].astype(f32) + ybuf[a, z].astype(f32)
        for way in range(2):
            before = has_l if way == 0 else has_r

            @pl.when(before)
            def _():
                arrived(zbuf.at[a, way, 0], rzr.at[a, way, 0])
                stage[a] += zbuf[a, way, 0].astype(f32)
        pltpu.make_async_copy(stage.at[a], (gup_hbm, gdown_hbm)[a], gosem.at[a]).start()

    def fetch(j):
        wcopy(j).wait()

        @pl.when(j + 2 < 2 * n_tiles)
        def _():
            wcopy(j + 2).start()

    def base_tiles(lo, hi):
        @pl.loop(lo, hi)
        def _(i):
            fetch(i)
            pbuf[i] = dot(xv[...], wbuf[i % 3]).astype(bf16)

            @pl.when(i % 2 == 0)
            def _():
                pd(i // 2).start()

    def grad_tiles(lo, hi):
        @pl.loop(lo, hi)
        def _(i):
            j = i + n_tiles
            fetch(j)

            @pl.when(i % 2 == 1)
            def _():
                gd_wait(i)
            for c in range(chunks):
                acc[:, c * tile:(c + 1) * tile] += dot(gbuf[i], wbuf[j % 3, c * tile:(c + 1) * tile, :], NT)

    def gforward(c):
        for k in range(1, big_k):
            gx(k, c).wait_recv()
            gd(k, c).start()

    def send_partial(c):
        for k in range(1, big_k):
            q = (k - 1) * chunks + c
            pd(q).wait_recv()
            pbuf[2 * q + 1] = (pbuf[2 * q + 1].astype(f32) + rbuf[q].astype(f32)).astype(bf16)
            px(k, c).start()

    def out_dx(c):
        cols = slice(c * tile, (c + 1) * tile)
        obuf[c % 2] = (acc[:, cols] + 2.0 * dot(wide[1], adp[0, :, cols], TN)).astype(bf16)
        pltpu.make_async_copy(obuf.at[c % 2], dx_hbm.at[:, pl.ds(c * tile, tile)], osem.at[c % 2]).start()

    def out_proj(c):
        cols = slice(c * tile, (c + 1) * tile)
        q = (big_k - 1) * chunks + c
        pd(q).wait_recv()
        total = pbuf[2 * q + 1].astype(f32) + rbuf[q].astype(f32) + 2.0 * dot(wide[0], adp[1, :, cols], TN)
        for k in range(1, big_k):
            px(k, c).wait_recv()
            total = total + xbuf[(k - 1) * chunks + c].astype(f32)
        obuf[c % 2] = total.astype(bf16)
        pltpu.make_async_copy(obuf.at[c % 2], proj_hbm.at[:, pl.ds(c * tile, tile)], osem.at[c % 2]).start()

    def out_wait(ref, c):
        pltpu.make_async_copy(obuf.at[c % 2], ref.at[:, pl.ds(c * tile, tile)], osem.at[c % 2]).wait()

    aload(0).start()
    aload(1).start()
    xload().start()
    wcopy(0).start()
    wcopy(1).start()
    for c in range(chunks):
        gload(c).start()

    barrier = pltpu.get_barrier_semaphore()
    pl.semaphore_signal(barrier, inc=1, device_id=partner, device_id_type=MESH)
    pl.semaphore_signal(barrier, inc=1, device_id=ypeer, device_id_type=MESH)
    for k in range(1, big_k):
        pl.semaphore_signal(barrier, inc=1, device_id=xpeer(k), device_id_type=MESH)

    @pl.when(has_l)
    def _():
        pl.semaphore_signal(barrier, inc=1, device_id=left, device_id_type=MESH)

    @pl.when(has_r)
    def _():
        pl.semaphore_signal(barrier, inc=1, device_id=right, device_id_type=MESH)
    pl.semaphore_wait(barrier, big_k + 1 + has_l.astype(jnp.int32) + has_r.astype(jnp.int32))

    early = max(1, chunks - 1)
    for c in range(early):
        for k in range(1, big_k):
            gx(k, c).start()
    aload(0).wait()
    adp[0, block(yc, z), :] = stage[0].astype(bf16)
    gather(0, 0)
    for c in range(chunks):
        gd(0, c).start()
    aload(1).wait()
    adp[1, block(yc, z), :] = stage[1].astype(bf16)

    tenants = counts_ref.shape[1]
    e = lax.broadcasted_iota(jnp.int32, (e_all, tenants), 0).astype(f32) + 0.5
    place = jnp.floor(e / e_own)
    col = jnp.floor((place + 0.5) / big_r)
    owner = (place - col * big_r) * 2.0 + col
    slot = owner * owned + jnp.floor((e - place * e_own) / rank)
    ids = lax.broadcasted_iota(jnp.int32, (e_all, tenants), 1).astype(f32)
    counts = jnp.broadcast_to(counts_ref[...].astype(f32), (e_all, tenants))
    match = jnp.broadcast_to(storage_ref[...].astype(f32), (e_all, tenants)) == slot
    mine = jnp.sum(jnp.where(match, ids, 0.0), axis=1, keepdims=True)
    bounds[0] = jnp.sum(jnp.where(ids < mine, counts, 0.0), axis=1, keepdims=True)
    bounds[1] = jnp.sum(jnp.where(ids <= mine, counts, 0.0), axis=1, keepdims=True)
    acc[...] = jnp.zeros_like(acc)
    xload().wait()

    cuts = [n_tiles * i // 8 for i in range(9)]
    base_tiles(0, cuts[2])
    gather(0, 1)
    gather(1, 0)
    base_tiles(cuts[2], cuts[4])
    for s in range(2, big_r - 1):
        gather(0, s)
    gforward(0)
    base_tiles(cuts[4], cuts[6])
    gather(0, big_r - 1)
    gather(1, 1)
    base_tiles(cuts[6], cuts[8])
    narrow(0)
    for c in range(chunks):
        gload(c).wait()
    grad_tiles(0, cuts[1])
    exchange(0)
    for c in range(early, chunks):
        for k in range(1, big_k):
            gx(k, c).start()
    for s in range(2, big_r - 1):
        gather(1, s)
    if chunks > 1:
        gforward(1)
    grad_tiles(cuts[1], cuts[2])
    gather(1, big_r - 1)
    send_partial(0)
    grad_tiles(cuts[2], cuts[3])
    spread(0)
    reduce_start(0)
    grad_tiles(cuts[3], cuts[4])
    for c in range(2, chunks):
        gforward(c)
    narrow(1)
    exchange(1)
    for c in range(1, chunks):
        send_partial(c)
    grad_tiles(cuts[4], cuts[5])
    for s in range(big_r - 1, big_r // 2, -1):
        reduce_step(0, s)
    spread(1)
    reduce_start(1)
    grad_tiles(cuts[5], cuts[6])
    for s in range(big_r // 2, 0, -1):
        reduce_step(0, s)
    reduce_end(0)
    grad_tiles(cuts[6], cuts[8])
    reduce_step(1, big_r - 1)
    for c in range(chunks):
        if c >= 2:
            out_wait(dx_hbm, c - 2)
        out_dx(c)
    for s in range(big_r - 2, 0, -1):
        reduce_step(1, s)
    for c in range(max(0, chunks - 2), chunks):
        out_wait(dx_hbm, c)
    for c in range(chunks - 1):
        if c >= 2:
            out_wait(proj_hbm, c - 2)
        out_proj(c)
    reduce_end(1)
    if chunks >= 3:
        out_wait(proj_hbm, chunks - 3)
    out_proj(chunks - 1)

    for k in range(1, big_k):
        for c in range(chunks):
            gx(k, c).wait_send()
            px(k, c).wait_send()
    for k in range(big_k):
        for c in range(chunks):
            gd(k, c).wait_send()
    for q in range(n_tiles // 2):
        pd(q).wait_send()
    for a in range(2):
        ed(a).wait_send()
        for k in range(1, big_k):
            exc(a, k).wait_send()
        for r in range(big_r):
            ay(a, r).wait_send()
            ry(a, r).wait_send()
        for way in range(2):
            to_has = has_r if way == 0 else has_l
            for s in range(big_r - 1):
                @pl.when(to_has & (z - s >= 0 if way == 0 else z + s < big_r))
                def _():
                    az(a, way, s).wait_send()

                @pl.when(z + s + 1 < big_r if way == 0 else z - s - 1 >= 0)
                def _():
                    rz(a, way, s + 1).wait_send()
        pltpu.make_async_copy(stage.at[a], (gup_hbm, gdown_hbm)[a], gosem.at[a]).wait()
    for c in range(max(0, chunks - 2), chunks):
        out_wait(proj_hbm, c)


def fused_step(n_dp, n_tensor, rank, x, w, g, down, up, counts, storage):
    f32, bf16 = jnp.float32, jnp.bfloat16
    rows, width = x.shape
    tile = min(512, width)
    chunks = width // tile
    n_tiles = n_tensor * chunks
    e_own = down.shape[0]
    e_all = e_own * n_dp
    big_r, big_k = n_dp // 2, n_tensor // 2
    far = max(1, big_k - 1)
    dma = pltpu.SemaphoreType.DMA
    any_spec, vmem_spec = pl.BlockSpec(memory_space=pl.ANY), pl.BlockSpec(memory_space=pltpu.VMEM)
    flops = 2 * rows * width * (2 * n_tiles * tile + 6 * e_all)
    return pl.pallas_call(
        functools.partial(step_kernel, n_dp, n_tensor, rank, tile),
        out_shape=(
            jax.ShapeDtypeStruct((rows, width), bf16),
            jax.ShapeDtypeStruct((rows, width), bf16),
            jax.ShapeDtypeStruct((e_own, width), f32),
            jax.ShapeDtypeStruct((e_own, width), f32),
        ),
        in_specs=[any_spec] * 5 + [vmem_spec] * 2,
        out_specs=(any_spec,) * 4,
        scratch_shapes=[
            pltpu.VMEM((rows, width), bf16),
            pltpu.VMEM((3, width, tile), bf16),
            pltpu.VMEM((n_tiles, rows, tile), bf16),
            pltpu.VMEM((n_tiles, rows, tile), bf16),
            pltpu.VMEM((n_tiles // 2, rows, tile), bf16),
            pltpu.VMEM((far * chunks, rows, tile), bf16),
            pltpu.VMEM((rows, width), f32),
            pltpu.VMEM((2, e_own, width), f32),
            pltpu.VMEM((2, e_all, width), bf16),
            pltpu.VMEM((2, e_all, rows), bf16),
            pltpu.VMEM((2, e_all, 1), f32),
            pltpu.VMEM((2, rank, rows), f32),
            pltpu.VMEM((2, rank, rows), f32),
            pltpu.VMEM((2, rank, rows), f32),
            pltpu.VMEM((2, far, rank, rows), f32),
            pltpu.VMEM((2, e_all, width), bf16),
            pltpu.VMEM((2, big_r, e_own, width), bf16),
            pltpu.VMEM((2, 2, big_r - 1, e_own, width), bf16),
            pltpu.VMEM((2, rows, tile), bf16),
            dma((3,)), dma, dma((chunks,)), dma((2,)), dma((2,)), dma((2,)),
            dma((far, chunks)), dma((far, chunks)),
            dma((big_k, chunks)), dma((big_k, chunks)),
            dma((n_tiles // 2,)), dma((n_tiles // 2,)),
            dma((far * chunks,)), dma((far * chunks,)),
            dma((2, 2, big_r - 1)), dma((2, 2, big_r - 1)),
            dma((2, big_r)), dma((2, big_r)),
            dma((2,)), dma((2,)), dma((2, far)), dma((2, far)),
            dma((2, big_r)), dma((2, big_r)),
            dma((2, 2, big_r - 1)), dma((2, 2, big_r - 1)),
        ],
        compiler_params=pltpu.CompilerParams(
            collective_id=0, has_side_effects=True, vmem_limit_bytes=67043328
        ),
        cost_estimate=pl.CostEstimate(flops=flops, bytes_accessed=2 * w.size * 2, transcendentals=0),
        name="fused_step",
    )(x, w, g, down, up, counts, storage)


def local(
    n_dp,
    n_tensor,
    attention_output,
    frozen_weight,
    output_gradient,
    tenant_token_count,
    tenant_storage_slot,
    adapter_down_weight,
    adapter_up_weight,
    down_first_moment,
    down_second_moment,
    up_first_moment,
    up_second_moment,
):
    width = attention_output.shape[1]
    owned, _, rank = adapter_down_weight.shape
    down = jnp.transpose(adapter_down_weight, (0, 2, 1)).reshape(owned * rank, width)
    up = adapter_up_weight.reshape(owned * rank, width)
    proj_out, input_grad, grad_up, grad_down = fused_step(
        n_dp, n_tensor, rank, attention_output, frozen_weight, output_gradient, down, up,
        tenant_token_count, tenant_storage_slot[None, :],
    )
    down_gradient = jnp.transpose(grad_down.reshape(owned, rank, width), (0, 2, 1))
    up_gradient = grad_up.reshape(owned, rank, width)
    updated_down_weight, updated_down_first_moment, updated_down_second_moment = adam_update(
        adapter_down_weight, down_first_moment, down_second_moment, down_gradient
    )
    updated_up_weight, updated_up_first_moment, updated_up_second_moment = adam_update(
        adapter_up_weight, up_first_moment, up_second_moment, up_gradient
    )
    return (
        proj_out,
        input_grad,
        updated_down_weight,
        updated_up_weight,
        updated_down_first_moment,
        updated_down_second_moment,
        updated_up_first_moment,
        updated_up_second_moment,
    )


def solution(mesh):
    wide, tall = P("dp", "tensor", None), P("dp", None, "tensor")
    return jax.shard_map(
        functools.partial(local, mesh.shape["dp"], mesh.shape["tensor"]),
        mesh=mesh,
        in_specs=(
            P("dp", "tensor"), P("tensor", None), P("dp", "tensor"), P("dp", None), P(),
            wide, tall, wide, wide, tall, tall,
        ),
        out_specs=(P("dp", "tensor"), P("dp", "tensor"), wide, tall, wide, wide, tall, tall),
        check_vma=False,
    )
```

```python
import functools

import jax
import jax.numpy as jnp
from jax import lax
from jax.experimental import pallas as pl
from jax.experimental.pallas import tpu as pltpu
from jax.sharding import PartitionSpec as P

MESH = pl.DeviceIdType.MESH
NT = (((1,), (1,)), ((), ()))
TN = (((0,), (0,)), ((), ()))


def adam_update(param, first, second, grad):
    first = 0.9 * first + 0.1 * grad
    second = 0.999 * second + 0.001 * grad * grad
    corr_one = 1.0 - 0.9**10
    corr_two = 1.0 - 0.999**10
    step_size = first / corr_one / (jnp.sqrt(second / corr_two) + 1e-08)
    return (param - 0.01 * (step_size + 0.1 * param), first, second)


def dot(a, b, dims=(((1,), (0,)), ((), ()))):
    return lax.dot_general(a, b, dims, preferred_element_type=jnp.float32)


def step_kernel(
    n_dp, n_tensor, rank, tile,
    x_hbm, w_hbm, g_hbm, down_hbm, up_hbm, counts_ref, storage_ref,
    proj_hbm, dx_hbm, gup_hbm, gdown_hbm,
    xv, wbuf, gbuf, pbuf, rbuf, xbuf, acc, stage, adp, wide, bounds,
    eown, epart, esum, ex, part, ybuf, zbuf, obuf,
    tbuf, sums, nbuf,
    wsem, xsem, glsem, alsem, osem, gosem, rts, rtr, rns, rnr,
    gxs, gxr, gds, gdr, pds, pdr, pxs, pxr,
    azs, azr, ays, ayr, eds, edr, exs, exr, rys, ryr, rzs, rzr,
):
    f32, bf16 = jnp.float32, jnp.bfloat16
    rows, width = x_hbm.shape
    chunks = width // tile
    n_tiles = n_tensor * chunks
    big_r, big_k = n_dp // 2, n_tensor // 2
    e_all, _ = adp.shape[1:]
    e_own = stage.shape[1]
    half = big_r * e_own
    owned = e_own // rank

    d, t = lax.axis_index("dp"), lax.axis_index("tensor")
    z, yc = d // 2, d % 2
    trow, core = t // 2, t % 2
    partner = (d, t + 1 - 2 * core)
    ypeer = (d + 1 - 2 * yc, t)
    left, right = (d - 2, t), (d + 2, t)
    has_l, has_r = z > 0, z < big_r - 1

    def xpeer(k):
        return (d, ((trow + k) % big_k) * 2 + core)

    def rc(src, dst, ss, rs, dev):
        return pltpu.make_async_remote_copy(
            src_ref=src, dst_ref=dst, send_sem=ss, recv_sem=rs, device_id=dev, device_id_type=MESH
        )

    def arrived(ref, sem):
        rc(ref, ref, sem, sem, partner).wait_recv()

    def tile_of(j):
        q = (j % n_tiles) // 2
        k, c, odd = q // chunks, q % chunks, j % 2
        base_row, base_core = (trow + k + 1) % big_k, jnp.where(odd == 0, 1 - core, core)
        grad_row, grad_core = (trow - k + big_k) % big_k, jnp.where(odd == 0, core, 1 - core)
        row = jnp.where(j < n_tiles, base_row, grad_row)
        side = jnp.where(j < n_tiles, base_core, grad_core)
        return (row * 2 + side) * chunks + c

    def wcopy(j):
        col = pl.multiple_of(tile_of(j) * tile, tile)
        return pltpu.make_async_copy(w_hbm.at[:, pl.ds(col, tile)], wbuf.at[j % 3], wsem.at[j % 3])

    def xload():
        return pltpu.make_async_copy(x_hbm, xv, xsem)

    def gload(c):
        return pltpu.make_async_copy(g_hbm.at[:, pl.ds(c * tile, tile)], gbuf.at[2 * c], glsem.at[c])

    def aload(a):
        return pltpu.make_async_copy((down_hbm, up_hbm)[a], stage.at[a], alsem.at[a])

    def piece(h):
        return pl.ds(h * (rows // 2), rows // 2)

    def gx(k, c, h):
        return rc(g_hbm.at[piece(h), pl.ds(c * tile, tile)], gbuf.at[(k * chunks + c) * 2, piece(h)],
                  gxs.at[k - 1, c, h], gxr.at[k - 1, c, h], xpeer(k))

    def gx_start(lo, hi):
        for n in range(lo, hi):
            for k in range(1, big_k):
                gx(k, n // 2, n % 2).start()

    def gd(k, c):
        slot = (k * chunks + c) * 2
        src = g_hbm.at[:, pl.ds(c * tile, tile)] if isinstance(k, int) and k == 0 else gbuf.at[slot]
        return rc(src, gbuf.at[slot + 1], gds.at[k, c], gdr.at[k, c], partner)

    def gd_wait(i):
        q = i // 2
        arrived(gbuf.at[i], gdr.at[q // chunks, q % chunks])

    def pd(q):
        return rc(pbuf.at[2 * q], rbuf.at[q], pds.at[q], pdr.at[q], partner)

    def px(k, c, h):
        q = (k - 1) * chunks + c
        return rc(pbuf.at[2 * q + 1, piece(h)], xbuf.at[q, piece(h)], pxs.at[q, h], pxr.at[q, h], xpeer(k))

    def block(col, row):
        return pl.ds(pl.multiple_of((col * big_r + row) * e_own, e_own), e_own)

    def az(a, way, s):
        row = z - s if way == 0 else z + s
        ref = adp.at[a, block(yc, row)]
        return rc(ref, ref, azs.at[a, way, s], azr.at[a, way, s], right if way == 0 else left)

    def ay(a, row):
        ref = adp.at[a, block(yc, row)]
        return rc(ref, ref, ays.at[a, row], ayr.at[a, row], ypeer)

    def ed(a):
        return rc(eown.at[a], epart.at[a], eds.at[a], edr.at[a], partner)

    def exc(a, k):
        return rc(esum.at[a], ex.at[a, k - 1], exs.at[a, k - 1], exr.at[a, k - 1], xpeer(k))

    def ry(a, row):
        return rc(part.at[a, block(1 - yc, row)], ybuf.at[a, row], rys.at[a, row], ryr.at[a, row], ypeer)

    def rz(a, way, s):
        row = z + s if way == 0 else z - s
        return rc(part.at[a, block(yc, row)], zbuf.at[a, way, s - 1],
                  rzs.at[a, way, s - 1], rzr.at[a, way, s - 1], (row * 2 + yc, t))

    near = jnp.where(z % 2 == 0, z + 1, z - 1)

    def target(way, s):
        row = z + s if way == 0 else z - s
        return (row < big_r if way == 0 else row >= 0), row, row != near

    def gather(a, s):
        for way in range(2):
            from_has = z - s >= 0 if way == 0 else z + s < big_r
            to_has = has_r if way == 0 else has_l
            row = z - s if way == 0 else z + s

            @pl.when(from_has)
            def _():
                if s > 0:
                    arrived(adp.at[a, block(yc, row)], azr.at[a, way, s - 1])
                if s < big_r - 1:
                    @pl.when(to_has)
                    def _():
                        az(a, way, s).start()
                if s > 0:
                    ay(a, row).start()

    def mask():
        tok = lax.broadcasted_iota(jnp.int32, (e_all, rows), 1).astype(f32)
        return (bounds[0] <= tok) & (tok < bounds[1])

    def narrow(a):
        for r in range(big_r):
            arrived(adp.at[a, block(1 - yc, r)], ayr.at[a, r])
        if a == 0:
            every = dot(adp[0], xv[...], NT)
        else:
            every = dot(adp[1, :, 0:tile], gbuf[0], NT)
            for c in range(1, chunks):
                every = every + dot(adp[1, :, c * tile:(c + 1) * tile], gbuf[2 * c], NT)
        kept = jnp.where(mask(), every, 0.0).reshape(e_all // rank, rank, rows)
        eown[a] = jnp.sum(kept, axis=0)
        ed(a).start()

    def exchange(a):
        ed(a).wait_recv()
        esum[a] = eown[a] + epart[a]
        for k in range(1, big_k):
            exc(a, k).start()

    def spread(a):
        total = esum[a]
        for k in range(1, big_k):
            exc(a, k).wait_recv()
            total = total + ex[a, k - 1]
        tiled = jnp.broadcast_to(total[None], (e_all // rank, rank, rows)).reshape(e_all, rows)
        wide[a] = jnp.where(mask(), tiled, 0.0).astype(bf16)

    def partial(a, side):
        here = pl.ds(pl.multiple_of(side * half, half), half)
        lhs = wide[a, here, :]
        for c in range(chunks):
            rhs = gbuf[2 * c] if a == 0 else xv[:, c * tile:(c + 1) * tile]
            part[a, here, c * tile:(c + 1) * tile] = (2.0 * dot(lhs, rhs)).astype(bf16)

    def rt(a):
        return rc(part.at[a, block(1 - yc, near)], tbuf.at[a], rts.at[a], rtr.at[a], (near * 2 + yc, t))

    def reduce_start(a):
        partial(a, 1 - yc)
        if a == 0:
            rt(a).start()
        for s in range(big_r - 1, 0, -1):
            for way in range(2):
                there, row, over_y = target(way, s)

                @pl.when(there & over_y)
                def _():
                    ry(a, row).start()
        partial(a, yc)
        if a == 0:
            reduce_near(a)

    def reduce_near(a):
        if a == 1:
            rt(a).start()
        for way in range(2):
            @pl.when(z % 2 == way)
            def _():
                rz(a, way, 1).start()

    def reduce_own(a):
        rt(a).wait_recv()
        here = block(1 - yc, z)
        part[a, here, :] = (part[a, here, :].astype(f32) + tbuf[a].astype(f32)).astype(bf16)
        ry(a, z).start()

    def rn(a, way, s):
        row = z + s if way == 0 else z - s
        return rc(part.at[a, block(yc, row)], nbuf.at[a, way, s - 2],
                  rns.at[a, way, s - 2], rnr.at[a, way, s - 2], (near * 2 + yc, t))

    def reduce_step(a, s):
        for way in range(2):
            there, row, over_y = target(way, s)

            @pl.when(there & over_y)
            def _():
                here = block(yc, row)
                arrived(ybuf.at[a, row], ryr.at[a, row])
                part[a, here, :] = (part[a, here, :].astype(f32) + ybuf[a, row].astype(f32)).astype(bf16)
                if s > 1:
                    @pl.when(z % 2 == way)
                    def _():
                        rn(a, way, s).start()
                if s < big_r - 1:
                    @pl.when(z % 2 != way)
                    def _():
                        arrived(nbuf.at[a, way, s - 1], rnr.at[a, way, s - 1])
                        part[a, here, :] = (part[a, here, :].astype(f32)
                                            + nbuf[a, way, s - 1].astype(f32)).astype(bf16)
                        rz(a, way, s).start()

    def grad_out(a):
        return pltpu.make_async_copy(sums.at[a], (gup_hbm, gdown_hbm)[a], gosem.at[a])

    def reduce_end(a):
        arrived(ybuf.at[a, z], ryr.at[a, z])
        sums[a] = part[a, block(yc, z), :].astype(f32) + ybuf[a, z].astype(f32)
        for s in range(1, big_r):
            for way in range(2):
                source = z - s if way == 0 else z + s
                inside = source >= 0 if way == 0 else source < big_r

                @pl.when(inside & ((source == near) | (source % 2 != way)))
                def _():
                    arrived(zbuf.at[a, way, s - 1], rzr.at[a, way, s - 1])
                    sums[a] += zbuf[a, way, s - 1].astype(f32)
        grad_out(a).start()

    def fetch(j):
        wcopy(j).wait()

        @pl.when(j + 2 < 2 * n_tiles)
        def _():
            wcopy(j + 2).start()

    def base_tiles(lo, hi):
        @pl.loop(lo, hi)
        def _(i):
            fetch(i)
            pbuf[i] = dot(xv[...], wbuf[i % 3]).astype(bf16)

            @pl.when(i % 2 == 0)
            def _():
                pd(i // 2).start()

    def grad_tiles(lo, hi):
        @pl.loop(lo, hi)
        def _(i):
            j = i + n_tiles
            fetch(j)

            @pl.when(i % 2 == 1)
            def _():
                gd_wait(i)
            for c in range(chunks):
                acc[:, c * tile:(c + 1) * tile] += dot(gbuf[i], wbuf[j % 3, c * tile:(c + 1) * tile, :], NT)

    def gforward(c):
        for k in range(1, big_k):
            for h in range(2):
                gx(k, c, h).wait_recv()
            gd(k, c).start()

    def send_partial(c, halves):
        for k in range(1, big_k):
            q = (k - 1) * chunks + c
            if 0 in halves:
                pd(q).wait_recv()
                pbuf[2 * q + 1] = (pbuf[2 * q + 1].astype(f32) + rbuf[q].astype(f32)).astype(bf16)
            for h in halves:
                px(k, c, h).start()

    def out_dx(c):
        cols = slice(c * tile, (c + 1) * tile)
        obuf[c % 2] = (acc[:, cols] + 2.0 * dot(wide[1], adp[0, :, cols], TN)).astype(bf16)
        pltpu.make_async_copy(obuf.at[c % 2], dx_hbm.at[:, pl.ds(c * tile, tile)], osem.at[c % 2]).start()

    def out_proj(c):
        cols = slice(c * tile, (c + 1) * tile)
        q = (big_k - 1) * chunks + c
        pd(q).wait_recv()
        total = pbuf[2 * q + 1].astype(f32) + rbuf[q].astype(f32) + 2.0 * dot(wide[0], adp[1, :, cols], TN)
        for k in range(1, big_k):
            for h in range(2):
                px(k, c, h).wait_recv()
            total = total + xbuf[(k - 1) * chunks + c].astype(f32)
        obuf[c % 2] = total.astype(bf16)
        pltpu.make_async_copy(obuf.at[c % 2], proj_hbm.at[:, pl.ds(c * tile, tile)], osem.at[c % 2]).start()

    def out_wait(ref, c):
        pltpu.make_async_copy(obuf.at[c % 2], ref.at[:, pl.ds(c * tile, tile)], osem.at[c % 2]).wait()

    aload(0).start()
    aload(1).start()
    xload().start()
    wcopy(0).start()
    wcopy(1).start()
    for c in range(chunks):
        gload(c).start()

    barrier = pltpu.get_barrier_semaphore()
    pl.semaphore_signal(barrier, inc=1, device_id=partner, device_id_type=MESH)
    pl.semaphore_signal(barrier, inc=1, device_id=ypeer, device_id_type=MESH)
    for k in range(1, big_k):
        pl.semaphore_signal(barrier, inc=1, device_id=xpeer(k), device_id_type=MESH)

    for s in range(1, big_r):
        for way in range(2):
            there, row, _ = target(way, s)

            @pl.when(there)
            def _():
                pl.semaphore_signal(barrier, inc=1, device_id=(row * 2 + yc, t), device_id_type=MESH)
    pl.semaphore_wait(barrier, big_k + big_r)

    early = 6 * chunks // 4
    gx_start(0, early)
    aload(0).wait()
    adp[0, block(yc, z), :] = stage[0].astype(bf16)
    gather(0, 0)
    ay(0, z).start()
    for c in range(chunks):
        gd(0, c).start()
    aload(1).wait()
    adp[1, block(yc, z), :] = stage[1].astype(bf16)

    tenants = counts_ref.shape[1]
    e = lax.broadcasted_iota(jnp.int32, (e_all, tenants), 0).astype(f32) + 0.5
    place = jnp.floor(e / e_own)
    col = jnp.floor((place + 0.5) / big_r)
    owner = (place - col * big_r) * 2.0 + col
    slot = owner * owned + jnp.floor((e - place * e_own) / rank)
    ids = lax.broadcasted_iota(jnp.int32, (e_all, tenants), 1).astype(f32)
    counts = jnp.broadcast_to(counts_ref[...].astype(f32), (e_all, tenants))
    match = jnp.broadcast_to(storage_ref[...].astype(f32), (e_all, tenants)) == slot
    mine = jnp.sum(jnp.where(match, ids, 0.0), axis=1, keepdims=True)
    bounds[0] = jnp.sum(jnp.where(ids < mine, counts, 0.0), axis=1, keepdims=True)
    bounds[1] = jnp.sum(jnp.where(ids <= mine, counts, 0.0), axis=1, keepdims=True)
    acc[...] = jnp.zeros_like(acc)
    xload().wait()

    cuts = [n_tiles * i // 8 for i in range(9)]
    base_tiles(0, cuts[2])
    gather(0, 1)
    ay(1, z).start()
    base_tiles(cuts[2], cuts[4])
    for s in range(2, big_r - 1):
        gather(0, s)
    gather(1, 0)
    gforward(0)
    base_tiles(cuts[4], cuts[6])
    gather(0, big_r - 1)
    base_tiles(cuts[6], cuts[8])
    gather(1, 1)
    if chunks > 1:
        gforward(1)
    for c in range(chunks):
        gload(c).wait()
    grad_tiles(0, cuts[1])
    for s in range(2, big_r - 1):
        gather(1, s)
    narrow(0)
    grad_tiles(cuts[1], cuts[1] + 1)
    exchange(0)
    gx_start(early, 2 * chunks)
    send_partial(0, (0,))
    grad_tiles(cuts[1] + 1, cuts[3])
    spread(0)
    gather(1, big_r - 1)
    reduce_start(0)
    grad_tiles(cuts[3], cuts[4])
    for c in range(2, chunks - 1):
        gforward(c)
    reduce_own(0)
    narrow(1)
    grad_tiles(cuts[4], cuts[4] + 1)
    exchange(1)
    send_partial(0, (1,))
    for c in range(1, chunks):
        send_partial(c, (0, 1))
    if chunks > 2:
        gforward(chunks - 1)
    grad_tiles(cuts[4] + 1, cuts[5])
    spread(1)
    reduce_start(1)
    for s in range(big_r - 1, big_r // 2, -1):
        reduce_step(0, s)
    grad_tiles(cuts[5], cuts[6])
    grad_tiles(cuts[6], cuts[6] + 1)
    for s in range(big_r // 2, 1, -1):
        reduce_step(0, s)
    reduce_near(1)
    grad_tiles(cuts[6] + 1, cuts[8])
    reduce_step(0, 1)
    for c in range(chunks // 2):
        out_dx(c)
    for s in range(big_r - 1, big_r // 2, -1):
        reduce_step(1, s)
    for c in range(chunks // 2, chunks):
        if c >= 2:
            out_wait(dx_hbm, c - 2)
        out_dx(c)
    reduce_own(1)
    for s in range(big_r // 2, 1, -1):
        reduce_step(1, s)
    for c in range(max(0, chunks - 2), chunks):
        out_wait(dx_hbm, c)
    for c in range(chunks // 2):
        out_proj(c)
    reduce_step(1, 1)
    reduce_end(0)
    for c in range(chunks // 2, chunks - 1):
        if c >= 2:
            out_wait(proj_hbm, c - 2)
        out_proj(c)
    reduce_end(1)
    if chunks >= 3:
        out_wait(proj_hbm, chunks - 3)
    out_proj(chunks - 1)

    for k in range(1, big_k):
        for c in range(chunks):
            for h in range(2):
                gx(k, c, h).wait_send()
                px(k, c, h).wait_send()
    for k in range(big_k):
        for c in range(chunks):
            gd(k, c).wait_send()
    for q in range(n_tiles // 2):
        pd(q).wait_send()
    for a in range(2):
        ed(a).wait_send()
        for k in range(1, big_k):
            exc(a, k).wait_send()
        for r in range(big_r):
            ay(a, r).wait_send()

            @pl.when(r != near)
            def _():
                ry(a, r).wait_send()
        for way in range(2):
            to_has = has_r if way == 0 else has_l
            for s in range(big_r - 1):
                @pl.when(to_has & (z - s >= 0 if way == 0 else z + s < big_r))
                def _():
                    az(a, way, s).wait_send()

                there, row, far_row = target(way, s + 1)

                @pl.when(there & (jnp.logical_not(far_row) | (z % 2 != way)))
                def _():
                    rz(a, way, s + 1).wait_send()
                if s > 0:
                    @pl.when(there & far_row & (z % 2 == way))
                    def _():
                        rn(a, way, s + 1).wait_send()
        rt(a).wait_send()
        grad_out(a).wait()
    for c in range(max(0, chunks - 2), chunks):
        out_wait(proj_hbm, c)


def finish_kernel(*refs):
    ins, outs = refs[:10], refs[10:16]
    proj_out, dx_out, state, large, isem, lsem, osem, losem = refs[16:]
    proj_in, dx_in = ins[-2:]
    pieces = large.shape[1]
    size = large.shape[2]

    def load(a, i):
        return pltpu.make_async_copy(ins[4 * a + i], state.at[a, i], isem.at[a, i])

    def big(b, h, out):
        here = pl.ds(h * size, size)
        if out:
            return pltpu.make_async_copy(large.at[b, h], (proj_out, dx_out)[b].at[here], losem.at[b, h])
        return pltpu.make_async_copy((proj_in, dx_in)[b].at[here], large.at[b, h], lsem.at[b, h])

    def store(a, i):
        return pltpu.make_async_copy(state.at[a, i], outs[3 * a + i], osem.at[a, i])

    for a in range(2):
        for i in range(4):
            load(a, i).start()
    for b in range(2):
        for h in range(pieces):
            big(b, h, False).start()
    for a in range(2):
        for i in range(4):
            load(a, i).wait()
        new = adam_update(state[a, 0], state[a, 1], state[a, 2], state[a, 3])
        for i in range(3):
            state[a, i] = new[i]
            store(a, i).start()
    for b in range(2):
        for h in range(pieces):
            big(b, h, False).wait()
            big(b, h, True).start()
    for a in range(2):
        for i in range(3):
            store(a, i).wait()
    for b in range(2):
        for h in range(pieces):
            big(b, h, True).wait()


def finish(sets, proj, dx):
    f32 = jnp.float32
    e_own, width = sets[0].shape
    rows = proj.shape[0]
    dma = pltpu.SemaphoreType.DMA
    any_spec = pl.BlockSpec(memory_space=pl.ANY)
    return pl.pallas_call(
        finish_kernel,
        out_shape=(jax.ShapeDtypeStruct((e_own, width), f32),) * 6
        + (jax.ShapeDtypeStruct(proj.shape, proj.dtype),) * 2,
        in_specs=[any_spec] * 10,
        out_specs=(any_spec,) * 8,
        scratch_shapes=[
            pltpu.VMEM((2, 4, e_own, width), f32),
            pltpu.VMEM((2, 4, rows // 4, width), proj.dtype),
            dma((2, 4)), dma((2, 4)), dma((2, 3)), dma((2, 4)),
        ],
        compiler_params=pltpu.CompilerParams(vmem_limit_bytes=60 * 1024 * 1024),
        name="finish",
    )(*sets, proj, dx)


def fused_step(n_dp, n_tensor, rank, x, w, g, down, up, counts, storage):
    f32, bf16 = jnp.float32, jnp.bfloat16
    rows, width = x.shape
    tile = min(512, width)
    chunks = width // tile
    n_tiles = n_tensor * chunks
    e_own = down.shape[0]
    e_all = e_own * n_dp
    big_r, big_k = n_dp // 2, n_tensor // 2
    far = max(1, big_k - 1)
    dma = pltpu.SemaphoreType.DMA
    any_spec, vmem_spec = pl.BlockSpec(memory_space=pl.ANY), pl.BlockSpec(memory_space=pltpu.VMEM)
    flops = 2 * rows * width * (2 * n_tiles * tile + 6 * e_all)
    return pl.pallas_call(
        functools.partial(step_kernel, n_dp, n_tensor, rank, tile),
        out_shape=(
            jax.ShapeDtypeStruct((rows, width), bf16),
            jax.ShapeDtypeStruct((rows, width), bf16),
        ) + (jax.ShapeDtypeStruct((e_own, width), f32),) * 2,
        in_specs=[any_spec] * 5 + [vmem_spec] * 2,
        out_specs=(any_spec,) * 4,
        scratch_shapes=[
            pltpu.VMEM((rows, width), bf16),
            pltpu.VMEM((3, width, tile), bf16),
            pltpu.VMEM((n_tiles, rows, tile), bf16),
            pltpu.VMEM((n_tiles, rows, tile), bf16),
            pltpu.VMEM((n_tiles // 2, rows, tile), bf16),
            pltpu.VMEM((far * chunks, rows, tile), bf16),
            pltpu.VMEM((rows, width), f32),
            pltpu.VMEM((2, e_own, width), f32),
            pltpu.VMEM((2, e_all, width), bf16),
            pltpu.VMEM((2, e_all, rows), bf16),
            pltpu.VMEM((2, e_all, 1), f32),
            pltpu.VMEM((2, rank, rows), f32),
            pltpu.VMEM((2, rank, rows), f32),
            pltpu.VMEM((2, rank, rows), f32),
            pltpu.VMEM((2, far, rank, rows), f32),
            pltpu.VMEM((2, e_all, width), bf16),
            pltpu.VMEM((2, big_r, e_own, width), bf16),
            pltpu.VMEM((2, 2, big_r - 1, e_own, width), bf16),
            pltpu.VMEM((2, rows, tile), bf16),
            pltpu.VMEM((2, e_own, width), bf16),
            pltpu.VMEM((2, e_own, width), f32),
            pltpu.VMEM((2, 2, big_r - 2, e_own, width), bf16),
            dma((3,)), dma, dma((chunks,)), dma((2,)), dma((2,)), dma((2,)), dma((2,)), dma((2,)),
            dma((2, 2, big_r - 2)), dma((2, 2, big_r - 2)),
            dma((far, chunks, 2)), dma((far, chunks, 2)),
            dma((big_k, chunks)), dma((big_k, chunks)),
            dma((n_tiles // 2,)), dma((n_tiles // 2,)),
            dma((far * chunks, 2)), dma((far * chunks, 2)),
            dma((2, 2, big_r - 1)), dma((2, 2, big_r - 1)),
            dma((2, big_r)), dma((2, big_r)),
            dma((2,)), dma((2,)), dma((2, far)), dma((2, far)),
            dma((2, big_r)), dma((2, big_r)),
            dma((2, 2, big_r - 1)), dma((2, 2, big_r - 1)),
        ],
        compiler_params=pltpu.CompilerParams(
            collective_id=0, has_side_effects=True, vmem_limit_bytes=67043328
        ),
        cost_estimate=pl.CostEstimate(flops=flops, bytes_accessed=2 * w.size * 2, transcendentals=0),
        name="fused_step",
    )(x, w, g, down, up, counts, storage)


def local(
    n_dp,
    n_tensor,
    attention_output,
    frozen_weight,
    output_gradient,
    tenant_token_count,
    tenant_storage_slot,
    adapter_down_weight,
    adapter_up_weight,
    down_first_moment,
    down_second_moment,
    up_first_moment,
    up_second_moment,
):
    width = attention_output.shape[1]
    owned, _, rank = adapter_down_weight.shape
    def flat(value):
        return jnp.transpose(value, (0, 2, 1)).reshape(owned * rank, width)

    def tall(value):
        return jnp.transpose(value.reshape(owned, rank, width), (0, 2, 1))

    def rows_of(value):
        return value.reshape(owned * rank, width)

    down, up = flat(adapter_down_weight), rows_of(adapter_up_weight)
    proj_out, input_grad, grad_up, grad_down = fused_step(
        n_dp, n_tensor, rank, attention_output, frozen_weight, output_gradient, down, up,
        tenant_token_count, tenant_storage_slot[None, :],
    )
    sets = (
        down, flat(down_first_moment), flat(down_second_moment), grad_down,
        up, rows_of(up_first_moment), rows_of(up_second_moment), grad_up,
    )
    new_down, new_dm, new_dv, new_up, new_um, new_uv, proj_out, input_grad = finish(sets, proj_out, input_grad)
    shape = adapter_up_weight.shape
    return (
        proj_out, input_grad, tall(new_down), new_up.reshape(shape),
        tall(new_dm), tall(new_dv), new_um.reshape(shape), new_uv.reshape(shape),
    )


def solution(mesh):
    wide, tall = P("dp", "tensor", None), P("dp", None, "tensor")
    return jax.shard_map(
        functools.partial(local, mesh.shape["dp"], mesh.shape["tensor"]),
        mesh=mesh,
        in_specs=(
            P("dp", "tensor"), P("tensor", None), P("dp", "tensor"), P("dp", None), P(),
            wide, tall, wide, wide, tall, tall,
        ),
        out_specs=(P("dp", "tensor"), P("dp", "tensor"), wide, tall, wide, wide, tall, tall),
        check_vma=False,
    )
```
